32 devices in a mesh: row: 16 (over z, y, core), head: 2 (over x).
Axes of the slice: x: 2, y: 2, z: 4, core: 2. Of those that a mesh axis runs over, the one named last changes fastest.
Arguments:
- pair_input: bfloat16 [32, 32, 128], P(('row', 'head')), may hold values from -6 to 6
- cotangent: bfloat16 [32, 32, 128], P(('row', 'head')), may hold values from -6 to 6
- residue_mask: int32 [32], replicated, may hold values from 0 to 1, as said below
- norm_gain: float32 [2, 128], replicated, may hold values from 0.5 to 1.5
- norm_shift: float32 [2, 128], replicated, may hold values from -3 to 3
- proj_weights: bfloat16 [2, 4, 128, 128], replicated, may hold values from -0.5 to 0.5
- gate_bias: float32 [2, 128], replicated, may hold values from -4 to 4
- out_weights: bfloat16 [2, 128, 128], replicated, may hold values from -1.0546875 to 1.0546875
- bias_weights: bfloat16 [2, 128, 4], replicated, may hold values from -1.06066017 to 1.06066017
Outputs:
- pair_grad: float32 [32, 32, 128], P(('row', 'head'))
- proj_grad: float32 [2, 4, 128, 128], replicated
- gate_bias_grad: float32 [2, 128], replicated
- out_grad: float32 [2, 128, 128], replicated
- bias_weight_grad: float32 [2, 128, 4], replicated
- gain_grad: float32 [2, 128], replicated
- shift_grad: float32 [2, 128], replicated
The draws below stay inside these ranges and needn't reach their ends.
Inputs may be any that keep to these rules, and one draw needn't show every extreme that they name: `residue_mask`: 1 for the first residues of the crop and 0 for the padding after them; at least half of the 32 residues are 1.
All inputs are finite; a program needn't handle non-finite values.
Results may differ from the reference program's by a relative error of at most 0.02.
The reference program's roundings to bfloat16 on the way count: a program that leaves them out, or rounds other values in their place, can miss the bound.
Values may be sent and summed in bfloat16 or wider, within the bound.
A program may use at most 64 MiB of HBM per device.

```python
import math
import jax
import jax.numpy as jnp
from jax import lax

PAIR = 128
HEADS = 4
HDIM = 32
ROW_DEV = 1
NRES = 32
N_ROW = 16
N_HEAD = 2


def draw_residue_mask(key, part):
    length = jax.random.randint(key, (), NRES // 2, NRES + 1)
    return (jnp.arange(NRES) < length).astype(jnp.int32)


def draw_bias_weights(key, part):
    base = jnp.clip(jax.random.normal(key, (2, PAIR, HEADS), jnp.float32), -4.0, 4.0) / math.sqrt(PAIR)
    return base.astype(jnp.bfloat16)


def spiked(result, own_key, source, target, shards_of, factor):
    def block_of(dim):
        return (jnp.arange(result.shape[dim]) // (result.shape[dim] // shards_of)).reshape((-1,) + (1,) * (result.ndim - 1 - dim))

    first = jax.random.permutation(own_key, shards_of)[block_of(target)]
    other_side = (block_of(target) + shards_of // 2) % shards_of
    return jnp.where((block_of(source) == first) | (block_of(source) == other_side), factor * result, result)


def block_levels(key, shape, split, smallest, largest):
    factor_of, own = 1.0, jax.random.fold_in(key, 6)
    for dim, parts in split:
        steps = jnp.exp(jax.random.uniform(jax.random.fold_in(own, dim), (parts,), jnp.float32, smallest / len(split), largest / len(split)))
        factor_of = factor_of * jnp.repeat(steps, shape[dim] // parts).reshape([-1 if axis == dim else 1 for axis in range(len(shape))])
    return factor_of


def scatter_about(rng, shape, deviation, limit, pieces=(), kind=jnp.bfloat16):
    factor_of = block_levels(rng, shape, pieces, -0.22, 0.18) if pieces else 1.0
    values = jax.random.normal(rng, shape, jnp.float32) * deviation * factor_of
    return jnp.minimum(jnp.maximum(values, -limit), limit).astype(kind)


def gaussian_with(own_key, dims, spread, most, pieces, heavy, held_as=jnp.bfloat16):
    drawn = spread * jax.random.normal(own_key, dims, jnp.float32)
    if pieces:
        drawn = drawn * block_levels(own_key, dims, pieces, -0.22, 0.18)
    return jnp.clip(spiked(drawn, jax.random.fold_in(own_key, 3), *heavy), -most, most).astype(held_as)


def setup_inputs(seed: int = 0) -> dict:
    key_of = jax.random.split(jax.random.key(seed), 10)
    return {
        "pair_input": scatter_about(key_of[0], (NRES, NRES, PAIR), 1.0, 6.0, ((0, 32),)),
        "cotangent": gaussian_with(key_of[1], (NRES, NRES, PAIR), 1.0, 6.0, ((0, 32),), (0, 2, 32, 2.75)),
        "residue_mask": draw_residue_mask(jax.random.fold_in(key_of[9], 71), 0),
        "norm_gain": jnp.clip(1.0 + 0.1 * jax.random.normal(key_of[3], (2, PAIR), jnp.float32), 0.5, 1.5),
        "norm_shift": scatter_about(key_of[4], (2, PAIR), 0.5, 3.0, (), jnp.float32),
        "proj_weights": scatter_about(key_of[5], (2, 4, PAIR, HEADS * HDIM), PAIR ** -0.5, 0.5),
        "gate_bias": scatter_about(key_of[6], (2, HEADS * HDIM), 1.0, 4.0, (), jnp.float32),
        "out_weights": scatter_about(key_of[7], (2, HEADS * HDIM, PAIR), (2.0 / (HEADS * HDIM) ** 0.5), 1.0546875),
        "bias_weights": draw_bias_weights(jax.random.fold_in(key_of[9], 71), 0),
    }


EPS = 1e-05
MASKED = 1000000000.0

def as_float(values):
    return values.astype(jnp.float32)

def to_half(values):
    return lax.optimization_barrier(values.astype(jnp.bfloat16))

def layer_norm(values, norm_scale, norm_offset):
    floats = as_float(values)
    centred = floats - lax.optimization_barrier(jnp.mean(floats, axis=-1, keepdims=True))
    inverse = lax.rsqrt(lax.optimization_barrier(jnp.mean(centred * centred, axis=-1, keepdims=True)) + EPS)
    normed = centred * inverse
    return (normed, inverse, to_half(normed * norm_scale + norm_offset))

def norm_backward(grad_normal, normed, inverse, norm_scale):
    grad_hat = grad_normal * norm_scale
    first_mean = lax.optimization_barrier(jnp.mean(grad_hat, axis=-1, keepdims=True))
    second_mean = lax.optimization_barrier(jnp.mean(grad_hat * normed, axis=-1, keepdims=True))
    return inverse * (grad_hat - first_mean - normed * second_mean)

def softmax_rows(logits):
    shifted = logits - lax.optimization_barrier(jnp.max(logits, axis=-1, keepdims=True))
    weights = jnp.exp(shifted)
    return weights / lax.optimization_barrier(jnp.sum(weights, axis=-1, keepdims=True))

def triangle_block(pair_values, grad_output, key_bias, params):
    norm_scale, norm_offset, projection, gate_offset, out_proj, bias_proj = params
    query_scale = 1.0 / math.sqrt(HDIM)
    inner_width = HEADS * HDIM
    normed, inverse, normal_in = layer_norm(pair_values, norm_scale, norm_offset)
    pair_bias = as_float(to_half(jnp.einsum('jkc,ch->hjk', as_float(normal_in), as_float(bias_proj))))
    class_ids = jnp.arange(NRES) // ROW_DEV % N_HEAD
    class_hot = (class_ids[None, :] == jnp.arange(N_HEAD)[:, None]).astype(jnp.float32)
    split_shape = (HEADS, N_ROW, N_HEAD, ROW_DEV)

    def one_row(totals, inputs):
        row_in, row_grad = inputs
        queries = to_half(jnp.dot(row_in, projection[0], preferred_element_type=jnp.float32) * query_scale)
        key_rows = to_half(jnp.dot(row_in, projection[1], preferred_element_type=jnp.float32))
        value_rows = to_half(jnp.dot(row_in, projection[2], preferred_element_type=jnp.float32))
        gate_values = jax.nn.sigmoid(jnp.dot(row_in, projection[3], preferred_element_type=jnp.float32) + gate_offset)
        head_query = as_float(queries).reshape(NRES, HEADS, HDIM).transpose(1, 0, 2)
        head_key = as_float(key_rows).reshape(NRES, HEADS, HDIM).transpose(1, 0, 2)
        head_value = as_float(value_rows).reshape(NRES, HEADS, HDIM).transpose(1, 0, 2)
        logits = jnp.einsum('hjd,hkd->hjk', head_query, head_key) + pair_bias + key_bias
        soft_weights = softmax_rows(logits)
        weights_half = as_float(to_half(soft_weights))
        attended = jnp.einsum('hjk,hkd->jhd', weights_half, head_value).reshape(NRES, inner_width)
        gated_out = to_half(gate_values * attended)
        update = to_half(jnp.dot(gated_out, out_proj, preferred_element_type=jnp.float32))
        grad_gated = jnp.dot(row_grad, out_proj.T, preferred_element_type=jnp.float32)
        grad_att = to_half(grad_gated * gate_values)
        grad_pre = to_half(grad_gated * attended * gate_values * (1.0 - gate_values))
        head_grad = as_float(grad_att).reshape(NRES, HEADS, HDIM).transpose(1, 0, 2)
        grad_weights = jnp.einsum('hjd,hkd->hjk', head_grad, head_value)
        grad_logits = soft_weights * (grad_weights - lax.optimization_barrier(jnp.sum(soft_weights * grad_weights, axis=-1, keepdims=True)))
        logits_half = as_float(to_half(grad_logits))
        grad_queries = to_half(jnp.einsum('hjk,hkd->jhd', logits_half, head_key) * query_scale).reshape(NRES, inner_width)
        blocks_logit = logits_half.reshape(split_shape + (NRES,))
        blocks_query = head_query.reshape(split_shape + (HDIM,))
        blocks_weight = weights_half.reshape(split_shape + (NRES,))
        blocks_grad = head_grad.reshape(split_shape + (HDIM,))
        grad_keys = to_half(jnp.einsum('hbcsk,hbcsd->ckhd', blocks_logit, blocks_query)).reshape(N_HEAD, NRES, inner_width)
        grad_values = to_half(jnp.einsum('hbcsk,hbcsd->ckhd', blocks_weight, blocks_grad)).reshape(N_HEAD, NRES, inner_width)
        key_part = jnp.einsum('cke,fe->ckf', as_float(grad_keys), as_float(projection[1]))
        key_part = key_part + jnp.einsum('cke,fe->ckf', as_float(grad_values), as_float(projection[2]))
        query_part = jnp.dot(grad_queries, projection[0].T, preferred_element_type=jnp.float32)
        query_part = query_part + jnp.dot(grad_pre, projection[3].T, preferred_element_type=jnp.float32)
        partial_value = to_half(key_part + class_hot[:, :, None] * query_part[None])
        grad_row = lax.optimization_barrier(jnp.sum(as_float(partial_value), axis=0))
        bias_sum, grad_qw, grad_kw, grad_vw, grad_gw, grad_ow, grad_gate = totals
        new_totals = (bias_sum + grad_logits, grad_qw + jnp.dot(row_in.T, grad_queries, preferred_element_type=jnp.float32), grad_kw + jnp.einsum('nc,gne->ce', as_float(row_in), as_float(grad_keys)), grad_vw + jnp.einsum('nc,gne->ce', as_float(row_in), as_float(grad_values)), grad_gw + jnp.dot(row_in.T, grad_pre, preferred_element_type=jnp.float32), grad_ow + jnp.dot(gated_out.T, row_grad, preferred_element_type=jnp.float32), grad_gate + lax.optimization_barrier(jnp.sum(as_float(grad_pre), axis=0)))
        return (new_totals, (update, grad_row))
    initial = (jnp.zeros((HEADS, NRES, NRES), jnp.float32), jnp.zeros((PAIR, inner_width), jnp.float32), jnp.zeros((PAIR, inner_width), jnp.float32), jnp.zeros((PAIR, inner_width), jnp.float32), jnp.zeros((PAIR, inner_width), jnp.float32), jnp.zeros((inner_width, PAIR), jnp.float32), jnp.zeros((inner_width,), jnp.float32))
    totals, (updates, grad_rows) = lax.scan(one_row, initial, (normal_in, grad_output))
    bias_sum, grad_qw, grad_kw, grad_vw, grad_gw, grad_ow, grad_gate = totals
    bias_half = as_float(to_half(bias_sum))
    grad_normal = grad_rows + jnp.einsum('hjk,ch->jkc', bias_half, as_float(bias_proj))
    grad_bias_weights = jnp.einsum('jkc,hjk->ch', as_float(normal_in), bias_half)
    grad_pair = norm_backward(grad_normal, normed, inverse, norm_scale)
    grad_scale = lax.optimization_barrier(jnp.sum(grad_normal * normed, axis=(0, 1)))
    grad_offset = lax.optimization_barrier(jnp.sum(grad_normal, axis=(0, 1)))
    weight_grads = (jnp.stack([grad_qw, grad_kw, grad_vw, grad_gw]), grad_gate, grad_ow, grad_bias_weights, grad_scale, grad_offset)
    return (updates, grad_pair, weight_grads)

def reference(pair_input, cotangent, residue_mask, norm_gain, norm_shift, proj_weights, gate_bias, out_weights, bias_weights):
    key_bias = (as_float(residue_mask) - 1.0) * MASKED
    params = [(norm_gain[which], norm_shift[which], proj_weights[which], gate_bias[which], out_weights[which], bias_weights[which]) for which in range(2)]
    updates, unused_grad, unused_weights = triangle_block(pair_input, jnp.zeros_like(cotangent), key_bias, params[0])
    after_first = to_half(as_float(pair_input) + as_float(updates))
    flipped = jnp.transpose(after_first, (1, 0, 2))
    flipped_grad = jnp.transpose(cotangent, (1, 0, 2))
    unused_updates, end_block, end_weights = triangle_block(flipped, flipped_grad, key_bias, params[1])
    end_grad = jnp.transpose(to_half(end_block), (1, 0, 2))
    grad_after = as_float(cotangent) + as_float(end_grad)
    later_updates, start_block, start_weights = triangle_block(pair_input, to_half(grad_after), key_bias, params[0])
    pair_grad = grad_after + start_block
    stacked = [jnp.stack([start_part, end_part]) for start_part, end_part in zip(start_weights, end_weights)]
    return (pair_grad, stacked[0], stacked[1], stacked[2], stacked[3], stacked[4], stacked[5])
```

```python
import functools
import math

import jax
import jax.numpy as jnp
from jax import lax
from jax.experimental import pallas as pl
from jax.experimental.pallas import tpu as pltpu
from jax.sharding import PartitionSpec as P

EPS = 1e-05
MASKED = 1000000000.0


def layer_norm(values, norm_scale, norm_offset):
    floats = values.astype(jnp.float32)
    centred = floats - jnp.mean(floats, axis=-1, keepdims=True)
    inverse = lax.rsqrt(jnp.mean(centred * centred, axis=-1, keepdims=True) + EPS)
    normed = centred * inverse
    return (normed, inverse, (normed * norm_scale + norm_offset).astype(jnp.bfloat16))


def norm_backward(grad_normal, normed, inverse, norm_scale):
    grad_hat = grad_normal * norm_scale
    first_mean = jnp.mean(grad_hat, axis=-1, keepdims=True)
    second_mean = jnp.mean(grad_hat * normed, axis=-1, keepdims=True)
    return inverse * (grad_hat - first_mean - normed * second_mean)


def class_columns(values, head_index, row_count, head_count, slab_rows):
    leading = values.shape[0]
    shaped = values.reshape(leading, row_count, head_count, slab_rows, values.shape[-1])
    picked = lax.dynamic_index_in_dim(shaped, head_index, axis=2, keepdims=False)
    return picked.reshape(leading, row_count * slab_rows, values.shape[-1])


def forward_block(pair_rows, key_bias, params, layout):
    norm_scale, norm_offset, projection, gate_offset, out_proj, bias_proj = params
    slab_rows, row_count, head_count, head_index = layout
    head_total = bias_proj.shape[1]
    inner_width = projection.shape[2]
    head_size = inner_width // head_total
    query_scale = 1.0 / math.sqrt(head_size)
    normed, inverse, normal_own = layer_norm(pair_rows, norm_scale, norm_offset)
    normal_rows = lax.all_gather(normal_own, "head", axis=0, tiled=True)
    bias_own = jnp.einsum(
        "snc,ch->hsn", normal_own, bias_proj, preferred_element_type=jnp.float32
    ).astype(jnp.bfloat16)
    bias_query = lax.all_gather(bias_own, "row", axis=1, tiled=True)
    normal_query = class_columns(normal_rows, head_index, row_count, head_count, slab_rows)
    block_rows = normal_query.shape[0]
    query_count = normal_query.shape[1]
    key_count = normal_rows.shape[1]
    queries = (
        jnp.dot(normal_query, projection[0], preferred_element_type=jnp.float32) * query_scale
    ).astype(jnp.bfloat16)
    joined_weights = jnp.concatenate([projection[1], projection[2]], axis=1)
    key_value = jnp.dot(normal_rows, joined_weights, preferred_element_type=jnp.float32).astype(
        jnp.bfloat16
    )
    gate_values = jax.nn.sigmoid(
        jnp.dot(normal_query, projection[3], preferred_element_type=jnp.float32) + gate_offset
    )
    head_queries = queries.reshape(block_rows, query_count, head_total, head_size).transpose(
        2, 0, 1, 3
    )
    head_pairs = key_value.reshape(block_rows, key_count, 2, head_total, head_size).transpose(
        2, 3, 0, 1, 4
    )

    def attend(inputs):
        query_head, key_head, value_head, bias_head = inputs
        logits = jnp.einsum(
            "rqd,rnd->rqn", query_head, key_head, preferred_element_type=jnp.float32
        )
        logits = logits + bias_head.astype(jnp.float32)[None] + key_bias
        largest = jnp.max(logits, axis=-1, keepdims=True)
        weights = jnp.exp(logits - largest)
        total = jnp.sum(weights, axis=-1, keepdims=True)
        soft_weights = weights / total
        attended = jnp.einsum(
            "rqn,rnd->rqd",
            soft_weights.astype(jnp.bfloat16),
            value_head,
            preferred_element_type=jnp.float32,
        )
        return ((largest + jnp.log(total))[..., 0], attended)

    log_totals, attended = lax.map(attend, (head_queries, head_pairs[0], head_pairs[1], bias_query))
    attended = attended.transpose(1, 2, 0, 3).reshape(block_rows, query_count, inner_width)
    gated_out = (gate_values * attended).astype(jnp.bfloat16)
    update = jnp.dot(gated_out, out_proj, preferred_element_type=jnp.float32).astype(jnp.bfloat16)
    saved_state = (
        normed,
        inverse,
        normal_own,
        normal_rows,
        normal_query,
        head_queries,
        head_pairs,
        bias_query,
        gate_values,
        attended,
        gated_out,
        log_totals,
    )
    return (saved_state, update)


def backward_block(saved_state, grad_query, key_bias, params, layout):
    norm_scale, norm_offset, projection, gate_offset, out_proj, bias_proj = params
    slab_rows, row_count, head_count, head_index = layout
    (
        normed,
        inverse,
        normal_own,
        normal_rows,
        normal_query,
        head_queries,
        head_pairs,
        bias_query,
        gate_values,
        attended,
        gated_out,
        log_totals,
    ) = saved_state
    channels = normal_own.shape[2]
    head_total, block_rows, query_count, head_size = head_queries.shape
    key_count = normal_rows.shape[1]
    inner_width = head_total * head_size
    query_scale = 1.0 / math.sqrt(head_size)
    grad_gated = jnp.dot(grad_query, out_proj.T, preferred_element_type=jnp.float32)
    grad_att = (grad_gated * gate_values).astype(jnp.bfloat16)
    grad_pre = (grad_gated * attended * gate_values * (1.0 - gate_values)).astype(jnp.bfloat16)
    head_grads = grad_att.reshape(block_rows, query_count, head_total, head_size).transpose(
        2, 0, 1, 3
    )

    def differentiate(inputs):
        total_head, query_head, key_head, value_head, bias_head, grad_head = inputs
        logits = jnp.einsum(
            "rqd,rnd->rqn", query_head, key_head, preferred_element_type=jnp.float32
        )
        logits = logits + bias_head.astype(jnp.float32)[None] + key_bias
        soft_weights = jnp.exp(logits - total_head[..., None])
        grad_weights = jnp.einsum(
            "rqd,rnd->rqn", grad_head, value_head, preferred_element_type=jnp.float32
        )
        grad_logits = soft_weights * (
            grad_weights - jnp.sum(soft_weights * grad_weights, axis=-1, keepdims=True)
        )
        logits_half = grad_logits.astype(jnp.bfloat16)
        grad_queries = (
            jnp.einsum("rqn,rnd->rqd", logits_half, key_head, preferred_element_type=jnp.float32)
            * query_scale
        ).astype(jnp.bfloat16)
        grad_keys = jnp.einsum(
            "rqn,rqd->rnd", logits_half, query_head, preferred_element_type=jnp.float32
        ).astype(jnp.bfloat16)
        grad_values = jnp.einsum(
            "rqn,rqd->rnd",
            soft_weights.astype(jnp.bfloat16),
            grad_head,
            preferred_element_type=jnp.float32,
        ).astype(jnp.bfloat16)
        return (grad_queries, grad_keys, grad_values, jnp.sum(grad_logits, axis=0))

    grad_queries, grad_keys, grad_values, grad_bias = lax.map(
        differentiate,
        (log_totals, head_queries, head_pairs[0], head_pairs[1], bias_query, head_grads),
    )
    grad_queries = grad_queries.transpose(1, 2, 0, 3).reshape(block_rows, query_count, inner_width)
    key_weights = projection[1].reshape(channels, head_total, head_size).transpose(1, 2, 0)
    value_weights = projection[2].reshape(channels, head_total, head_size).transpose(1, 2, 0)
    query_side = jnp.dot(grad_queries, projection[0].T, preferred_element_type=jnp.float32)
    query_side = query_side + jnp.dot(grad_pre, projection[3].T, preferred_element_type=jnp.float32)
    count = slab_rows * lax.axis_size("head")
    term = jnp.einsum("hrnd,hdc->rnc", grad_keys, key_weights, preferred_element_type=jnp.float32)
    term = term + jnp.einsum(
        "hrnd,hdc->rnc", grad_values, value_weights, preferred_element_type=jnp.float32
    )
    shaped = term.reshape(count, row_count, head_count, slab_rows, channels)
    current = lax.dynamic_slice_in_dim(shaped, head_index, 1, 2)
    query_slice = query_side.reshape(count, row_count, 1, slab_rows, channels)
    shaped = lax.dynamic_update_slice_in_dim(shaped, current + query_slice, head_index, 2)
    grad_normal = lax.psum_scatter(
        shaped.reshape(count, key_count, channels).astype(jnp.bfloat16),
        "head",
        scatter_dimension=0,
        tiled=True,
    ).astype(jnp.float32)
    bias_total = lax.psum_scatter(grad_bias, "row", scatter_dimension=1, tiled=True)
    bias_half = bias_total.astype(jnp.bfloat16)
    grad_normal = grad_normal + jnp.einsum(
        "hsn,ch->snc", bias_half, bias_proj, preferred_element_type=jnp.float32
    )
    grad_pair = norm_backward(grad_normal, normed, inverse, norm_scale)
    projection_grads = jnp.stack(
        [
            jnp.einsum(
                "rqc,rqe->ce", normal_query, grad_queries, preferred_element_type=jnp.float32
            ),
            jnp.einsum(
                "rnc,hrnd->chd", normal_rows, grad_keys, preferred_element_type=jnp.float32
            ).reshape(channels, inner_width),
            jnp.einsum(
                "rnc,hrnd->chd", normal_rows, grad_values, preferred_element_type=jnp.float32
            ).reshape(channels, inner_width),
            jnp.einsum("rqc,rqe->ce", normal_query, grad_pre, preferred_element_type=jnp.float32),
        ]
    )
    weight_grads = (
        projection_grads,
        jnp.sum(grad_pre.astype(jnp.float32), axis=(0, 1)),
        jnp.einsum("rqe,rqc->ec", gated_out, grad_query, preferred_element_type=jnp.float32),
        jnp.einsum("snc,hsn->ch", normal_own, bias_half, preferred_element_type=jnp.float32),
        jnp.sum(grad_normal * normed, axis=(0, 1)),
        jnp.sum(grad_normal, axis=(0, 1)),
    )
    return (grad_pair, weight_grads)


def to_queries(grad_rows, layout):
    slab_rows, row_count, head_count, head_index = layout
    channels = grad_rows.shape[2]
    shaped = grad_rows.reshape(slab_rows, row_count, head_count, slab_rows, channels)
    moved = lax.all_to_all(shaped, "head", split_axis=2, concat_axis=0, tiled=True)
    return moved.reshape(slab_rows * head_count, row_count * slab_rows, channels)


def sum_side(weight_grads):
    return lax.psum(
        (
            weight_grads[0],
            weight_grads[1],
            weight_grads[2],
            weight_grads[3],
            weight_grads[4],
            weight_grads[5],
        ),
        ("row", "head"),
    )


def local(
    pair_input,
    cotangent,
    residue_mask,
    norm_gain,
    norm_shift,
    proj_weights,
    gate_bias,
    out_weights,
    bias_weights,
):
    slab_rows = pair_input.shape[0]
    channels = pair_input.shape[2]
    row_count = lax.axis_size("row")
    head_count = lax.axis_size("head")
    layout = (slab_rows, row_count, head_count, lax.axis_index("head"))
    key_bias = (residue_mask.astype(jnp.float32) - 1.0) * MASKED
    params = [
        (
            norm_gain[which],
            norm_shift[which],
            proj_weights[which],
            gate_bias[which],
            out_weights[which],
            bias_weights[which],
        )
        for which in range(2)
    ]
    first_state, first_update = forward_block(pair_input, key_bias, params[0], layout)
    returned = lax.all_to_all(
        first_update.reshape(slab_rows * head_count, row_count, 1, slab_rows, channels),
        "head",
        split_axis=0,
        concat_axis=2,
        tiled=True,
    )
    after_first = (
        pair_input.astype(jnp.float32)
        + returned.reshape(slab_rows, -1, channels).astype(jnp.float32)
    ).astype(jnp.bfloat16)
    joined = jnp.concatenate([after_first, cotangent], axis=2)
    moved = lax.all_to_all(
        lax.all_to_all(
            joined.reshape(1, 1, slab_rows, row_count, head_count, slab_rows, 2 * channels),
            "row",
            split_axis=3,
            concat_axis=0,
            tiled=True,
        ),
        "head",
        split_axis=4,
        concat_axis=1,
        tiled=True,
    )
    flipped = moved.reshape(-1, slab_rows, 2 * channels).transpose(1, 0, 2)
    second_state, second_update = forward_block(
        flipped[:, :, :channels], key_bias, params[1], layout
    )
    second_grad, second_weights = backward_block(
        second_state, to_queries(flipped[:, :, channels:], layout), key_bias, params[1], layout
    )
    second_weights = sum_side(second_weights)
    sent_back = lax.all_to_all(
        lax.all_to_all(
            second_grad.astype(jnp.bfloat16).reshape(
                1, 1, slab_rows, row_count, head_count, slab_rows, channels
            ),
            "row",
            split_axis=3,
            concat_axis=0,
            tiled=True,
        ),
        "head",
        split_axis=4,
        concat_axis=1,
        tiled=True,
    )
    end_grad = sent_back.reshape(-1, slab_rows, channels).transpose(1, 0, 2)
    grad_after = cotangent.astype(jnp.float32) + end_grad.astype(jnp.float32)
    start_grad, first_weights = backward_block(
        first_state,
        to_queries(grad_after.astype(jnp.bfloat16), layout),
        key_bias,
        params[0],
        layout,
    )
    pair_grad = grad_after + start_grad
    first_weights = sum_side(first_weights)
    stacked = [
        jnp.stack([start_part, end_part])
        for start_part, end_part in zip(first_weights, second_weights)
    ]
    return (pair_grad, stacked[0], stacked[1], stacked[2], stacked[3], stacked[4], stacked[5])


MESH = pl.DeviceIdType.MESH
F32 = jnp.float32
BF16 = jnp.bfloat16
TILE = 16
RESIDENT = 4
VMEM_GRANT = 16 * 1024 * 1024
NN = ((1,), (0,))
NT = ((1,), (1,))
TN = ((0,), (0,))


def mm(a, b, contract):
    return lax.dot_general(a, b, (contract, ((), ())), preferred_element_type=F32)


def bits_of(count):
    return range(count.bit_length() - 1)


def fused_kernel(
    n_head,
    held,
    group,
    heads,
    pair_far,
    cot_far,
    mask_far,
    gain_far,
    shift_far,
    proj_far,
    gate_far,
    out_far,
    bias_far,
    pair_out,
    weights_out,
    small_out,
    pair_ref,
    cot_ref,
    mask_ref,
    gain_ref,
    shift_ref,
    proj_ref,
    gate_ref,
    out_ref,
    bias_ref,
    stage_in,
    got_in,
    stage_bias,
    got_bias,
    stage_flip,
    got_flip,
    stage_bias1,
    got_bias1,
    stage_back,
    got_back,
    stage_sum,
    got_sum,
    stage_w,
    got_w,
    own_w,
    stage_small,
    got_small,
    result,
    send_sem,
    recv_sem,
    load_sem,
):
    row = lax.axis_index("row")
    head = lax.axis_index("head")
    me = row * n_head + head
    layer = me // group
    seat = me % group
    nres, channels = pair_ref.shape[1:]
    inner = proj_ref.shape[3]
    hdim = inner // heads
    wide = heads * nres
    cells = held * nres
    scale = 1.0 / math.sqrt(hdim)
    barrier = pltpu.get_barrier_semaphore()
    waits = []

    seat_steps = []
    for bit in bits_of(group):
        step = 1 << bit
        sign = 1 - 2 * (seat // step % 2)
        if step < n_head:
            seat_steps.append((sign * step, 0, sign * step))
        else:
            seat_steps.append((sign * step, sign * (step // n_head), 0))
    layer_steps = []
    for bit in bits_of(held):
        step = 1 << bit
        sign = 1 - 2 * (layer // step % 2)
        layer_steps.append((sign * step, sign * (step * (group // n_head)), 0))

    def partners(place, steps):
        found = []
        for flip in range((1 << len(steps)) - 1, 0, -1):
            chosen = [steps[i] for i in range(len(steps)) if flip >> i & 1]
            found.append(
                (
                    place + sum(part[0] for part in chosen),
                    (row + sum(part[1] for part in chosen), head + sum(part[2] for part in chosen)),
                )
            )
        return found

    mates = partners(seat, seat_steps)
    twins = partners(layer, layer_steps)

    def send(source_of, target, channel, slot=None, peers=mates, part=None):
        place = seat if slot is None else slot
        goal = target.at[place] if part is None else target.at[place, part]
        for other, device in peers:
            pltpu.make_async_remote_copy(
                src_ref=source_of(other),
                dst_ref=goal,
                send_sem=send_sem.at[channel],
                recv_sem=recv_sem.at[channel],
                device_id=device,
                device_id_type=MESH,
            ).start()
        waits.append((target, channel, part))

    def wait_all(target, sem, part=None):
        count = pl.ds(0, target.shape[0] - 1)
        view = target.at[count] if part is None else target.at[count, part]
        pltpu.make_async_copy(view, view, sem).wait()

    def received(target, channel, part=None):
        with jax.named_scope(f"w{channel}"):
            wait_all(target, recv_sem.at[channel], part)

    loads = {}
    for i, (name, far, near) in enumerate(
        (
            ("pair", pair_far, pair_ref),
            ("gain", gain_far, gain_ref),
            ("shift", shift_far, shift_ref),
            ("bias", bias_far, bias_ref),
            ("cot", cot_far, cot_ref),
            ("mask", mask_far, mask_ref),
            ("proj", proj_far, proj_ref),
            ("gate", gate_far, gate_ref),
            ("out", out_far, out_ref),
        )
    ):
        loads[name] = pltpu.make_async_copy(far, near, load_sem.at[i])
    loads["pair"].start()
    for other, device in twins + mates:
        pl.semaphore_signal(barrier, inc=1, device_id=device, device_id_type=MESH)
    for name in loads:
        if name != "pair":
            loads[name].start()

    def iota(shape, dim):
        return lax.broadcasted_iota(jnp.int32, shape, dim)

    def natural(position):
        return position % held * group + position // held

    head_mask = (iota((wide, inner), 0) // nres == iota((wide, inner), 1) // hdim).astype(F32)
    head_half = head_mask.astype(BF16)
    diagonal = (iota((nres, wide), 0) == iota((nres, wide), 1) % nres).astype(F32)
    order = natural(iota((nres, nres), 0)) == iota((nres, nres), 1)
    rows_of = iota((cells, cells), 0)
    cols_of = iota((cells, cells), 1)
    block = held * held
    pack = (
        rows_of % held * nres + rows_of // block * held + rows_of // held % held == cols_of
    ).astype(BF16)
    unpack = (
        rows_of // held % group * block + rows_of // nres * held + rows_of % held == cols_of
    ).astype(BF16)

    def expand(values):
        return jnp.concatenate([values] * heads, axis=0) * head_half

    def pick_heads(full):
        kept = full * head_mask
        total = kept[:nres]
        for h in range(1, heads):
            total = total + kept[h * nres : (h + 1) * nres]
        return total

    def flip_heads(values):
        turned = values.T
        return jnp.concatenate(
            [turned[h * nres : (h + 1) * nres] for h in range(heads)], axis=1
        )

    def wide_bias(which):
        rows = bias_ref[which].astype(F32)
        return jnp.concatenate(
            [jnp.broadcast_to(rows[h : h + 1], (nres, channels)) for h in range(heads)],
            axis=0,
        ).astype(BF16)

    def norm(values, which):
        return layer_norm(values, gain_ref[which : which + 1], shift_ref[which : which + 1])

    def split(values):
        return [values[r * nres : (r + 1) * nres] for r in range(held)]

    def bias_rows(normal, spread):
        full = mm(normal, spread, NT)
        rows = [jnp.sum(part * diagonal, axis=0, keepdims=True) for part in split(full)]
        return jnp.concatenate(rows, axis=0).astype(BF16).astype(F32)

    def project(normal, which):
        queries = (mm(normal, proj_ref[which, 0], NN) * scale).astype(BF16)
        keys = mm(normal, proj_ref[which, 1], NN).astype(BF16)
        values = mm(normal, proj_ref[which, 2], NN).astype(BF16)
        gate = jax.nn.sigmoid(
            mm(normal, proj_ref[which, 3], NN) + gate_ref[which : which + 1]
        )
        wide_queries = [expand(part) for part in split(queries)]
        key_parts = split(keys)
        logits = [mm(k, q, NT) + key_bias for k, q in zip(key_parts, wide_queries)]
        return key_parts, split(values), gate, wide_queries, logits

    def attend(parts, bias):
        keys, values, gate, wide_queries, logits = parts
        probs, halves, attended = [], [], []
        for r in range(held):
            scores = logits[r] + bias
            weights = jnp.exp(scores - jnp.max(scores, axis=0, keepdims=True))
            probs.append(weights / jnp.sum(weights, axis=0, keepdims=True))
            halves.append(probs[r].astype(BF16))
            attended.append(pick_heads(mm(halves[r], values[r], TN)))
        attended = jnp.concatenate(attended, axis=0)
        gated = (gate * attended).astype(BF16)
        return probs, halves, attended, gated

    def logit_grads(parts, soft, grad_gated):
        keys, values, gate, wide_queries, unused = parts
        probs, halves, attended, gated = soft
        wide_grads = [expand(part) for part in split((grad_gated * gate).astype(BF16))]
        grad_pre = (grad_gated * attended * gate * (1.0 - gate)).astype(BF16)
        bias_sum, logit_halves = None, []
        for r in range(held):
            grad_probs = mm(values[r], wide_grads[r], NT)
            grad_logits = probs[r] * (
                grad_probs - jnp.sum(probs[r] * grad_probs, axis=0, keepdims=True)
            )
            bias_sum = grad_logits if r == 0 else bias_sum + grad_logits
            logit_halves.append(grad_logits.astype(BF16))
        return bias_sum, (wide_grads, grad_pre, logit_halves)

    def cell_grads(parts, soft, found):
        keys, values, gate, wide_queries, unused = parts
        wide_grads, grad_pre, logit_halves = found
        halves = soft[1]
        queries_out, keys_out, values_out = [], [], []
        for r in range(held):
            queries_out.append((pick_heads(mm(logit_halves[r], keys[r], TN)) * scale).astype(BF16))
            keys_out.append(mm(logit_halves[r], wide_queries[r], NN).astype(BF16))
            values_out.append(mm(halves[r], wide_grads[r], NN).astype(BF16))
        return (
            jnp.concatenate(queries_out, axis=0),
            jnp.concatenate(keys_out, axis=0),
            jnp.concatenate(values_out, axis=0),
            grad_pre,
        )

    def join(grads, which):
        total = mm(grads[0], proj_ref[which, 0], NT)
        for m in range(1, 4):
            total = total + mm(grads[m], proj_ref[which, m], NT)
        return total

    def stage_matrix(slot, tile, matrix):
        half = matrix.astype(BF16)
        for r in range(matrix.shape[0] // TILE):
            stage_w[slot, tile % group, tile // group] = half[r * TILE : (r + 1) * TILE]
            tile += 1

    def stage_weights(normal, grads, gated, grad_out, slot):
        tiles = channels // TILE
        for m in range(4):
            stage_matrix(slot, m * tiles, mm(normal, grads[m], TN))
        stage_matrix(slot, 4 * tiles, mm(gated, grad_out, TN))

    def bias_back(normal, spread, total):
        rounded = total.astype(BF16).astype(F32)
        placed = jnp.concatenate(
            [rounded[r : r + 1] * diagonal for r in range(held)], axis=0
        ).astype(BF16)
        grown = mm(placed, spread, NN)
        by_cell = mm(placed, normal, TN)
        rows = [
            jnp.sum(by_cell[h * nres : (h + 1) * nres], axis=0, keepdims=True)
            for h in range(heads)
        ]
        return grown, rows

    def stage_sums(which, rows, grad_pre, grad_normal, normed):
        rows = rows + [
            jnp.sum(grad_pre.astype(F32), axis=0, keepdims=True),
            jnp.sum(grad_normal * normed, axis=0, keepdims=True),
            jnp.sum(grad_normal, axis=0, keepdims=True),
        ]
        spare = stage_small.shape[1] - len(rows)
        if spare:
            rows = rows + [jnp.zeros((spare, channels), F32)]
        stage_small[which] = jnp.concatenate(rows, axis=0)

    def reduce_weights(slot):
        total = jnp.sum(got_w[slot].astype(F32), axis=0).astype(BF16)
        own_w[slot] = total
        weights_out[slot, seat] = total

    order_half = order.astype(BF16)
    loads["pair"].wait()
    pair_own = mm(order_half, pair_ref[0], NN).astype(BF16)
    stage_in[0] = pair_own
    got_in[0, layer] = pair_own
    loads["cot"].wait()
    cot_own = mm(order_half, cot_ref[0], NN).astype(BF16)
    stage_in[1] = cot_own
    got_in[1, layer] = cot_own
    with jax.named_scope("bar"):
        pl.semaphore_wait(barrier, len(twins) + len(mates))
    send(lambda other: stage_in.at[0], got_in.at[0], 0, layer, twins)
    send(lambda other: stage_in.at[1], got_in.at[1], 12, layer, twins)
    for name in ("gain", "shift", "bias", "mask", "proj", "gate", "out"):
        loads[name].wait()
    key_row = (mask_ref[...].astype(F32) - 1.0) * MASKED
    key_bias = jnp.sum(jnp.where(order, key_row, 0.0), axis=1, keepdims=True)
    spread0 = wide_bias(0)
    spread1 = wide_bias(1)
    received(got_in.at[0], 0)
    first_in = got_in[0].reshape(cells, channels)
    normed0, inverse0, normal0 = norm(first_in, 0)
    row0 = bias_rows(normal0, spread0)
    stage_bias[...] = row0
    got_bias[seat] = row0
    send(lambda other: stage_bias, got_bias, 1)

    parts0 = project(normal0, 0)
    received(got_in.at[1], 12)
    cotangent_half = got_in[1].reshape(cells, channels)
    cotangent = cotangent_half.astype(F32)
    packed_grad = mm(pack, cotangent_half, NN).astype(BF16)
    received(got_bias, 1)
    soft0 = attend(parts0, flip_heads(got_bias[...].reshape(nres, wide)))
    update = mm(soft0[3], out_ref[0], NN).astype(BF16)
    after_first = (first_in.astype(F32) + update.astype(F32)).astype(BF16)
    packed = mm(pack, after_first, NN).astype(BF16)
    packed = jnp.concatenate([packed, packed_grad], axis=1).reshape(group, block, 2 * channels)
    stage_flip[...] = packed
    got_flip[seat] = stage_flip[seat]
    send(lambda other: stage_flip.at[other], got_flip, 2)
    normed1, inverse1, normal1 = norm(after_first, 1)
    row1 = bias_rows(normal1, spread1)
    stage_bias1[...] = row1
    got_bias1[seat] = row1
    send(lambda other: stage_bias1, got_bias1, 3)
    received(got_flip, 2)

    flipped = mm(unpack, got_flip[...].reshape(cells, 2 * channels), NN).astype(BF16)
    column_grad = flipped[:, channels:]
    unused_normed, unused_inverse, normal_col = norm(flipped[:, :channels], 1)
    parts1 = project(normal_col, 1)
    grad_gated1 = mm(column_grad, out_ref[1], NT)
    received(got_bias1, 3)
    soft1 = attend(parts1, got_bias1[...].reshape(nres, wide))
    bias_sum1, found1 = logit_grads(parts1, soft1, grad_gated1)
    stage_sum[1] = bias_sum1.reshape(group, held, wide)
    got_sum[1, seat] = stage_sum[1, seat]
    send(lambda other: stage_sum.at[1, other], got_sum.at[1], 4)
    grads1 = cell_grads(parts1, soft1, found1)
    back = mm(pack, join(grads1, 1).astype(BF16), NN).astype(BF16)
    stage_back[...] = back.reshape(group, block, channels)
    got_back[seat] = stage_back[seat]
    send(lambda other: stage_back.at[other], got_back, 5)
    stage_weights(normal_col, grads1, soft1[3], column_grad, 1)
    got_w[1, seat] = stage_w[1, seat]
    send(lambda other: stage_w.at[1, other], got_w.at[1], 6)
    received(got_sum.at[1], 4)
    grown1, rows1 = bias_back(normal1, spread1, jnp.sum(got_sum[1], axis=0))
    received(got_back, 5)
    back = mm(unpack, got_back[...].reshape(cells, channels), NN)
    grad_normal1 = back + grown1
    end_grad = norm_backward(grad_normal1, normed1, inverse1, gain_ref[1:2])
    grad_after = cotangent + end_grad.astype(BF16).astype(F32)
    grad_after_half = grad_after.astype(BF16)

    grad_gated0 = mm(grad_after_half, out_ref[0], NT)
    bias_sum0, found0 = logit_grads(parts0, soft0, grad_gated0)
    stage_sum[0] = flip_heads(bias_sum0).reshape(group, held, wide)
    got_sum[0, seat] = stage_sum[0, seat]
    send(lambda other: stage_sum.at[0, other], got_sum.at[0], 7)
    received(got_w.at[1], 6)
    reduce_weights(1)
    send(lambda other: own_w.at[1], weights_out.at[1], 9)
    grads0 = cell_grads(parts0, soft0, found0)
    stage_weights(normal0, grads0, soft0[3], grad_after_half, 0)
    got_w[0, seat] = stage_w[0, seat]
    send(lambda other: stage_w.at[0, other], got_w.at[0], 8)
    stage_sums(1, rows1, grads1[3], grad_normal1, normed1)
    joined0 = join(grads0, 0)
    received(got_sum.at[0], 7)
    grown0, rows0 = bias_back(normal0, spread0, jnp.sum(got_sum[0], axis=0))
    grad_normal0 = grown0 + joined0
    stage_sums(0, rows0, grads0[3], grad_normal0, normed0)
    got_small[seat] = stage_small[...]
    send(lambda other: stage_small, got_small, 10)
    start_grad = norm_backward(grad_normal0, normed0, inverse0, gain_ref[0:1])
    result[...] = (grad_after + start_grad).reshape(held, nres, channels)
    received(got_w.at[0], 8)
    reduce_weights(0)
    send(lambda other: own_w.at[0], weights_out.at[0], 11)
    kept = result[layer]
    for p in range(nres):
        i = p % held * group + p // held
        pair_out[0, i : i + 1] = kept[p : p + 1]
    received(weights_out.at[1], 9)
    received(got_small, 10)
    small_out[...] = jnp.sum(got_small[...], axis=0)
    received(weights_out.at[0], 11)
    with jax.named_scope("ends"):
        for target, channel, part in waits:
            wait_all(target, send_sem.at[channel], part)


def finish_kernel(
    heads,
    pair_in,
    weights_in,
    small_in,
    pair_out,
    proj_out,
    gate_out,
    outw_out,
    biasw_out,
    gain_out,
    shift_out,
):
    group = weights_in.shape[1]
    pair_out[...] = pair_in[...]
    for which in range(2):
        tile = 0
        for m in range(5):
            for r in range(proj_out.shape[2] // TILE):
                piece = weights_in[which, tile % group, tile // group].astype(F32)
                if m < 4:
                    proj_out[which, m, r * TILE : (r + 1) * TILE] = piece
                else:
                    outw_out[which, r * TILE : (r + 1) * TILE] = piece
                tile += 1
        small = small_in[which]
        biasw_out[which] = small[:heads]
        gate_out[which : which + 1] = small[heads : heads + 1]
        gain_out[which : which + 1] = small[heads + 1 : heads + 2]
        shift_out[which : which + 1] = small[heads + 2 : heads + 3]


def fused(
    row_count,
    head_count,
    pair_input,
    cotangent,
    residue_mask,
    norm_gain,
    norm_shift,
    proj_weights,
    gate_bias,
    out_weights,
    bias_weights,
):
    n = row_count * head_count
    held = RESIDENT
    group = n // held
    nres, channels = pair_input.shape[1:]
    heads = bias_weights.shape[2]
    slots = 5 * channels // TILE // group
    wide = heads * nres
    block = held * held
    small = -(-(heads + 3) // 8) * 8
    shape = jax.ShapeDtypeStruct
    vmem = pl.BlockSpec(memory_space=pltpu.VMEM)
    far = pl.BlockSpec(memory_space=pltpu.HBM)
    inputs = (
        pair_input,
        cotangent,
        residue_mask.reshape(1, -1),
        norm_gain,
        norm_shift,
        proj_weights,
        gate_bias,
        out_weights,
        bias_weights.transpose(0, 2, 1),
    )
    parts = pl.pallas_call(
        functools.partial(fused_kernel, head_count, held, group, heads),
        out_shape=(
            shape(pair_input.shape, F32),
            shape((2, group, slots, TILE, channels), BF16),
            shape((2, small, channels), F32),
        ),
        in_specs=[far] * len(inputs),
        out_specs=[vmem] * 3,
        scratch_shapes=[pltpu.VMEM(each.shape, each.dtype) for each in inputs]
        + [
            pltpu.VMEM((2, nres, channels), BF16),
            pltpu.VMEM((2, held, nres, channels), BF16),
            pltpu.VMEM((held, wide), F32),
            pltpu.VMEM((group, held, wide), F32),
            pltpu.VMEM((group, block, 2 * channels), BF16),
            pltpu.VMEM((group, block, 2 * channels), BF16),
            pltpu.VMEM((held, wide), F32),
            pltpu.VMEM((group, held, wide), F32),
            pltpu.VMEM((group, block, channels), BF16),
            pltpu.VMEM((group, block, channels), BF16),
            pltpu.VMEM((2, group, held, wide), F32),
            pltpu.VMEM((2, group, held, wide), F32),
            pltpu.VMEM((2, group, slots, TILE, channels), BF16),
            pltpu.VMEM((2, group, slots, TILE, channels), BF16),
            pltpu.VMEM((2, slots, TILE, channels), BF16),
            pltpu.VMEM((2, small, channels), F32),
            pltpu.VMEM((group, 2, small, channels), F32),
            pltpu.VMEM((held, nres, channels), F32),
            pltpu.SemaphoreType.DMA((13,)),
            pltpu.SemaphoreType.DMA((13,)),
            pltpu.SemaphoreType.DMA((len(inputs),)),
        ],
        compiler_params=pltpu.CompilerParams(
            collective_id=0, has_side_effects=True, vmem_limit_bytes=VMEM_GRANT
        ),
    )(*(pltpu.with_memory_space_constraint(each, pltpu.HBM) for each in inputs))
    outs = pl.pallas_call(
        functools.partial(finish_kernel, heads),
        out_shape=(
            shape(pair_input.shape, F32),
            shape(proj_weights.shape, F32),
            shape(gate_bias.shape, F32),
            shape(out_weights.shape, F32),
            shape((2, heads, channels), F32),
            shape(norm_gain.shape, F32),
            shape(norm_shift.shape, F32),
        ),
        in_specs=[vmem] * 3,
        out_specs=[vmem] * 7,
        compiler_params=pltpu.CompilerParams(vmem_limit_bytes=VMEM_GRANT),
    )(*parts)
    outs = list(outs)
    outs[4] = outs[4].transpose(0, 2, 1)
    return tuple(outs)


def dispatch(row_count, head_count, *arrays):
    pair_input, proj_weights, bias_weights = arrays[0], arrays[5], arrays[8]
    rows, residues, channels = pair_input.shape
    inner = proj_weights.shape[3]
    wide = bias_weights.shape[2] * residues
    group = row_count * head_count // RESIDENT
    fits = (
        rows == 1
        and residues == group * RESIDENT
        and wide == inner == channels
        and 5 * channels % (TILE * group) == 0
        and group & (group - 1) == 0
        and group % head_count == 0
    )
    if fits:
        return fused(row_count, head_count, *arrays)
    return local(*arrays)


def solution(mesh):
    return jax.shard_map(
        functools.partial(dispatch, mesh.shape["row"], mesh.shape["head"]),
        mesh=mesh,
        in_specs=(
            P(("row", "head"), None, None),
            P(("row", "head"), None, None),
            P(),
            P(),
            P(),
            P(),
            P(),
            P(),
            P(),
        ),
        out_specs=(P(("row", "head"), None, None), P(), P(), P(), P(), P(), P()),
        check_vma=False,
    )
```

```python
import functools
import math

import jax
import jax.numpy as jnp
from jax import lax
from jax.experimental import pallas as pl
from jax.experimental.pallas import tpu as pltpu
from jax.sharding import PartitionSpec as P

EPS = 1e-05
MASKED = 1000000000.0


def layer_norm(values, norm_scale, norm_offset):
    floats = values.astype(jnp.float32)
    centred = floats - jnp.mean(floats, axis=-1, keepdims=True)
    inverse = lax.rsqrt(jnp.mean(centred * centred, axis=-1, keepdims=True) + EPS)
    normed = centred * inverse
    return (normed, inverse, (normed * norm_scale + norm_offset).astype(jnp.bfloat16))


def norm_backward(grad_normal, normed, inverse, norm_scale):
    grad_hat = grad_normal * norm_scale
    first_mean = jnp.mean(grad_hat, axis=-1, keepdims=True)
    second_mean = jnp.mean(grad_hat * normed, axis=-1, keepdims=True)
    return inverse * (grad_hat - first_mean - normed * second_mean)


def class_columns(values, head_index, row_count, head_count, slab_rows):
    leading = values.shape[0]
    shaped = values.reshape(leading, row_count, head_count, slab_rows, values.shape[-1])
    picked = lax.dynamic_index_in_dim(shaped, head_index, axis=2, keepdims=False)
    return picked.reshape(leading, row_count * slab_rows, values.shape[-1])


def forward_block(pair_rows, key_bias, params, layout):
    norm_scale, norm_offset, projection, gate_offset, out_proj, bias_proj = params
    slab_rows, row_count, head_count, head_index = layout
    head_total = bias_proj.shape[1]
    inner_width = projection.shape[2]
    head_size = inner_width // head_total
    query_scale = 1.0 / math.sqrt(head_size)
    normed, inverse, normal_own = layer_norm(pair_rows, norm_scale, norm_offset)
    normal_rows = lax.all_gather(normal_own, "head", axis=0, tiled=True)
    bias_own = jnp.einsum(
        "snc,ch->hsn", normal_own, bias_proj, preferred_element_type=jnp.float32
    ).astype(jnp.bfloat16)
    bias_query = lax.all_gather(bias_own, "row", axis=1, tiled=True)
    normal_query = class_columns(normal_rows, head_index, row_count, head_count, slab_rows)
    block_rows = normal_query.shape[0]
    query_count = normal_query.shape[1]
    key_count = normal_rows.shape[1]
    queries = (
        jnp.dot(normal_query, projection[0], preferred_element_type=jnp.float32) * query_scale
    ).astype(jnp.bfloat16)
    joined_weights = jnp.concatenate([projection[1], projection[2]], axis=1)
    key_value = jnp.dot(normal_rows, joined_weights, preferred_element_type=jnp.float32).astype(
        jnp.bfloat16
    )
    gate_values = jax.nn.sigmoid(
        jnp.dot(normal_query, projection[3], preferred_element_type=jnp.float32) + gate_offset
    )
    head_queries = queries.reshape(block_rows, query_count, head_total, head_size).transpose(
        2, 0, 1, 3
    )
    head_pairs = key_value.reshape(block_rows, key_count, 2, head_total, head_size).transpose(
        2, 3, 0, 1, 4
    )

    def attend(inputs):
        query_head, key_head, value_head, bias_head = inputs
        logits = jnp.einsum(
            "rqd,rnd->rqn", query_head, key_head, preferred_element_type=jnp.float32
        )
        logits = logits + bias_head.astype(jnp.float32)[None] + key_bias
        largest = jnp.max(logits, axis=-1, keepdims=True)
        weights = jnp.exp(logits - largest)
        total = jnp.sum(weights, axis=-1, keepdims=True)
        soft_weights = weights / total
        attended = jnp.einsum(
            "rqn,rnd->rqd",
            soft_weights.astype(jnp.bfloat16),
            value_head,
            preferred_element_type=jnp.float32,
        )
        return ((largest + jnp.log(total))[..., 0], attended)

    log_totals, attended = lax.map(attend, (head_queries, head_pairs[0], head_pairs[1], bias_query))
    attended = attended.transpose(1, 2, 0, 3).reshape(block_rows, query_count, inner_width)
    gated_out = (gate_values * attended).astype(jnp.bfloat16)
    update = jnp.dot(gated_out, out_proj, preferred_element_type=jnp.float32).astype(jnp.bfloat16)
    saved_state = (
        normed,
        inverse,
        normal_own,
        normal_rows,
        normal_query,
        head_queries,
        head_pairs,
        bias_query,
        gate_values,
        attended,
        gated_out,
        log_totals,
    )
    return (saved_state, update)


def backward_block(saved_state, grad_query, key_bias, params, layout):
    norm_scale, norm_offset, projection, gate_offset, out_proj, bias_proj = params
    slab_rows, row_count, head_count, head_index = layout
    (
        normed,
        inverse,
        normal_own,
        normal_rows,
        normal_query,
        head_queries,
        head_pairs,
        bias_query,
        gate_values,
        attended,
        gated_out,
        log_totals,
    ) = saved_state
    channels = normal_own.shape[2]
    head_total, block_rows, query_count, head_size = head_queries.shape
    key_count = normal_rows.shape[1]
    inner_width = head_total * head_size
    query_scale = 1.0 / math.sqrt(head_size)
    grad_gated = jnp.dot(grad_query, out_proj.T, preferred_element_type=jnp.float32)
    grad_att = (grad_gated * gate_values).astype(jnp.bfloat16)
    grad_pre = (grad_gated * attended * gate_values * (1.0 - gate_values)).astype(jnp.bfloat16)
    head_grads = grad_att.reshape(block_rows, query_count, head_total, head_size).transpose(
        2, 0, 1, 3
    )

    def differentiate(inputs):
        total_head, query_head, key_head, value_head, bias_head, grad_head = inputs
        logits = jnp.einsum(
            "rqd,rnd->rqn", query_head, key_head, preferred_element_type=jnp.float32
        )
        logits = logits + bias_head.astype(jnp.float32)[None] + key_bias
        soft_weights = jnp.exp(logits - total_head[..., None])
        grad_weights = jnp.einsum(
            "rqd,rnd->rqn", grad_head, value_head, preferred_element_type=jnp.float32
        )
        grad_logits = soft_weights * (
            grad_weights - jnp.sum(soft_weights * grad_weights, axis=-1, keepdims=True)
        )
        logits_half = grad_logits.astype(jnp.bfloat16)
        grad_queries = (
            jnp.einsum("rqn,rnd->rqd", logits_half, key_head, preferred_element_type=jnp.float32)
            * query_scale
        ).astype(jnp.bfloat16)
        grad_keys = jnp.einsum(
            "rqn,rqd->rnd", logits_half, query_head, preferred_element_type=jnp.float32
        ).astype(jnp.bfloat16)
        grad_values = jnp.einsum(
            "rqn,rqd->rnd",
            soft_weights.astype(jnp.bfloat16),
            grad_head,
            preferred_element_type=jnp.float32,
        ).astype(jnp.bfloat16)
        return (grad_queries, grad_keys, grad_values, jnp.sum(grad_logits, axis=0))

    grad_queries, grad_keys, grad_values, grad_bias = lax.map(
        differentiate,
        (log_totals, head_queries, head_pairs[0], head_pairs[1], bias_query, head_grads),
    )
    grad_queries = grad_queries.transpose(1, 2, 0, 3).reshape(block_rows, query_count, inner_width)
    key_weights = projection[1].reshape(channels, head_total, head_size).transpose(1, 2, 0)
    value_weights = projection[2].reshape(channels, head_total, head_size).transpose(1, 2, 0)
    query_side = jnp.dot(grad_queries, projection[0].T, preferred_element_type=jnp.float32)
    query_side = query_side + jnp.dot(grad_pre, projection[3].T, preferred_element_type=jnp.float32)
    count = slab_rows * lax.axis_size("head")
    term = jnp.einsum("hrnd,hdc->rnc", grad_keys, key_weights, preferred_element_type=jnp.float32)
    term = term + jnp.einsum(
        "hrnd,hdc->rnc", grad_values, value_weights, preferred_element_type=jnp.float32
    )
    shaped = term.reshape(count, row_count, head_count, slab_rows, channels)
    current = lax.dynamic_slice_in_dim(shaped, head_index, 1, 2)
    query_slice = query_side.reshape(count, row_count, 1, slab_rows, channels)
    shaped = lax.dynamic_update_slice_in_dim(shaped, current + query_slice, head_index, 2)
    grad_normal = lax.psum_scatter(
        shaped.reshape(count, key_count, channels).astype(jnp.bfloat16),
        "head",
        scatter_dimension=0,
        tiled=True,
    ).astype(jnp.float32)
    bias_total = lax.psum_scatter(grad_bias, "row", scatter_dimension=1, tiled=True)
    bias_half = bias_total.astype(jnp.bfloat16)
    grad_normal = grad_normal + jnp.einsum(
        "hsn,ch->snc", bias_half, bias_proj, preferred_element_type=jnp.float32
    )
    grad_pair = norm_backward(grad_normal, normed, inverse, norm_scale)
    projection_grads = jnp.stack(
        [
            jnp.einsum(
                "rqc,rqe->ce", normal_query, grad_queries, preferred_element_type=jnp.float32
            ),
            jnp.einsum(
                "rnc,hrnd->chd", normal_rows, grad_keys, preferred_element_type=jnp.float32
            ).reshape(channels, inner_width),
            jnp.einsum(
                "rnc,hrnd->chd", normal_rows, grad_values, preferred_element_type=jnp.float32
            ).reshape(channels, inner_width),
            jnp.einsum("rqc,rqe->ce", normal_query, grad_pre, preferred_element_type=jnp.float32),
        ]
    )
    weight_grads = (
        projection_grads,
        jnp.sum(grad_pre.astype(jnp.float32), axis=(0, 1)),
        jnp.einsum("rqe,rqc->ec", gated_out, grad_query, preferred_element_type=jnp.float32),
        jnp.einsum("snc,hsn->ch", normal_own, bias_half, preferred_element_type=jnp.float32),
        jnp.sum(grad_normal * normed, axis=(0, 1)),
        jnp.sum(grad_normal, axis=(0, 1)),
    )
    return (grad_pair, weight_grads)


def to_queries(grad_rows, layout):
    slab_rows, row_count, head_count, head_index = layout
    channels = grad_rows.shape[2]
    shaped = grad_rows.reshape(slab_rows, row_count, head_count, slab_rows, channels)
    moved = lax.all_to_all(shaped, "head", split_axis=2, concat_axis=0, tiled=True)
    return moved.reshape(slab_rows * head_count, row_count * slab_rows, channels)


def sum_side(weight_grads):
    return lax.psum(
        (
            weight_grads[0],
            weight_grads[1],
            weight_grads[2],
            weight_grads[3],
            weight_grads[4],
            weight_grads[5],
        ),
        ("row", "head"),
    )


def local(
    pair_input,
    cotangent,
    residue_mask,
    norm_gain,
    norm_shift,
    proj_weights,
    gate_bias,
    out_weights,
    bias_weights,
):
    slab_rows = pair_input.shape[0]
    channels = pair_input.shape[2]
    row_count = lax.axis_size("row")
    head_count = lax.axis_size("head")
    layout = (slab_rows, row_count, head_count, lax.axis_index("head"))
    key_bias = (residue_mask.astype(jnp.float32) - 1.0) * MASKED
    params = [
        (
            norm_gain[which],
            norm_shift[which],
            proj_weights[which],
            gate_bias[which],
            out_weights[which],
            bias_weights[which],
        )
        for which in range(2)
    ]
    first_state, first_update = forward_block(pair_input, key_bias, params[0], layout)
    returned = lax.all_to_all(
        first_update.reshape(slab_rows * head_count, row_count, 1, slab_rows, channels),
        "head",
        split_axis=0,
        concat_axis=2,
        tiled=True,
    )
    after_first = (
        pair_input.astype(jnp.float32)
        + returned.reshape(slab_rows, -1, channels).astype(jnp.float32)
    ).astype(jnp.bfloat16)
    joined = jnp.concatenate([after_first, cotangent], axis=2)
    moved = lax.all_to_all(
        lax.all_to_all(
            joined.reshape(1, 1, slab_rows, row_count, head_count, slab_rows, 2 * channels),
            "row",
            split_axis=3,
            concat_axis=0,
            tiled=True,
        ),
        "head",
        split_axis=4,
        concat_axis=1,
        tiled=True,
    )
    flipped = moved.reshape(-1, slab_rows, 2 * channels).transpose(1, 0, 2)
    second_state, second_update = forward_block(
        flipped[:, :, :channels], key_bias, params[1], layout
    )
    second_grad, second_weights = backward_block(
        second_state, to_queries(flipped[:, :, channels:], layout), key_bias, params[1], layout
    )
    second_weights = sum_side(second_weights)
    sent_back = lax.all_to_all(
        lax.all_to_all(
            second_grad.astype(jnp.bfloat16).reshape(
                1, 1, slab_rows, row_count, head_count, slab_rows, channels
            ),
            "row",
            split_axis=3,
            concat_axis=0,
            tiled=True,
        ),
        "head",
        split_axis=4,
        concat_axis=1,
        tiled=True,
    )
    end_grad = sent_back.reshape(-1, slab_rows, channels).transpose(1, 0, 2)
    grad_after = cotangent.astype(jnp.float32) + end_grad.astype(jnp.float32)
    start_grad, first_weights = backward_block(
        first_state,
        to_queries(grad_after.astype(jnp.bfloat16), layout),
        key_bias,
        params[0],
        layout,
    )
    pair_grad = grad_after + start_grad
    first_weights = sum_side(first_weights)
    stacked = [
        jnp.stack([start_part, end_part])
        for start_part, end_part in zip(first_weights, second_weights)
    ]
    return (pair_grad, stacked[0], stacked[1], stacked[2], stacked[3], stacked[4], stacked[5])


MESH = pl.DeviceIdType.MESH
F32 = jnp.float32
BF16 = jnp.bfloat16
TILE = 16
RESIDENT = 4
VMEM_GRANT = 16 * 1024 * 1024
NN = ((1,), (0,))
NT = ((1,), (1,))
TN = ((0,), (0,))


def mm(a, b, contract):
    return lax.dot_general(a, b, (contract, ((), ())), preferred_element_type=F32)


def bits_of(count):
    return range(count.bit_length() - 1)


def fused_kernel(
    n_head,
    held,
    group,
    heads,
    pair_far,
    cot_far,
    mask_far,
    gain_far,
    shift_far,
    proj_far,
    gate_far,
    out_far,
    bias_far,
    pair_out,
    weights_out,
    small_out,
    pair_ref,
    cot_ref,
    mask_ref,
    gain_ref,
    shift_ref,
    proj_ref,
    gate_ref,
    out_ref,
    bias_ref,
    stage_in,
    got_in,
    stage_bias,
    got_bias,
    stage_flip,
    got_flip,
    stage_bias1,
    got_bias1,
    stage_back,
    got_back,
    stage_sum,
    got_sum,
    stage_w,
    got_w,
    own_w,
    stage_small,
    got_small,
    result,
    send_sem,
    recv_sem,
    load_sem,
):
    row = lax.axis_index("row")
    head = lax.axis_index("head")
    me = row * n_head + head
    layer = me // group
    seat = me % group
    nres, channels = pair_ref.shape[1:]
    inner = proj_ref.shape[3]
    hdim = inner // heads
    wide = heads * nres
    cells = held * nres
    scale = 1.0 / math.sqrt(hdim)
    barrier = pltpu.get_barrier_semaphore()
    waits = []

    seat_steps = []
    for bit in bits_of(group):
        step = 1 << bit
        sign = 1 - 2 * (seat // step % 2)
        if step < n_head:
            seat_steps.append((sign * step, 0, sign * step))
        else:
            seat_steps.append((sign * step, sign * (step // n_head), 0))
    layer_steps = []
    for bit in bits_of(held):
        step = 1 << bit
        sign = 1 - 2 * (layer // step % 2)
        layer_steps.append((sign * step, sign * (step * (group // n_head)), 0))

    def partners(place, steps):
        found = []
        for flip in range((1 << len(steps)) - 1, 0, -1):
            chosen = [steps[i] for i in range(len(steps)) if flip >> i & 1]
            found.append(
                (
                    place + sum(part[0] for part in chosen),
                    (row + sum(part[1] for part in chosen), head + sum(part[2] for part in chosen)),
                )
            )
        return found

    mates = partners(seat, seat_steps)
    twins = partners(layer, layer_steps)
    others = partners(0, seat_steps + layer_steps)

    def send(source_of, target, channel, slot=None, peers=mates, part=None):
        place = seat if slot is None else slot
        goal = target.at[place] if part is None else target.at[place, part]
        for other, device in peers:
            pltpu.make_async_remote_copy(
                src_ref=source_of(other),
                dst_ref=goal,
                send_sem=send_sem.at[channel],
                recv_sem=recv_sem.at[channel],
                device_id=device,
                device_id_type=MESH,
            ).start()
        waits.append((target, channel, part))

    def wait_all(target, sem, part=None):
        count = pl.ds(0, target.shape[0] - 1)
        view = target.at[count] if part is None else target.at[count, part]
        pltpu.make_async_copy(view, view, sem).wait()

    def received(target, channel, part=None):
        with jax.named_scope(f"w{channel}"):
            wait_all(target, recv_sem.at[channel], part)

    loads = {}
    for i, (name, far, near) in enumerate(
        (
            ("pair", pair_far, pair_ref),
            ("gain", gain_far, gain_ref),
            ("shift", shift_far, shift_ref),
            ("bias", bias_far, bias_ref),
            ("cot", cot_far, cot_ref),
            ("mask", mask_far, mask_ref),
            ("proj", proj_far, proj_ref),
            ("gate", gate_far, gate_ref),
            ("out", out_far, out_ref),
        )
    ):
        loads[name] = pltpu.make_async_copy(far, near, load_sem.at[i])
    loads["pair"].start()
    for other, device in others:
        pl.semaphore_signal(barrier, inc=1, device_id=device, device_id_type=MESH)
    for name in loads:
        if name != "pair":
            loads[name].start()

    def iota(shape, dim):
        return lax.broadcasted_iota(jnp.int32, shape, dim)

    def natural(position):
        return position % held * group + position // held

    head_mask = (iota((wide, inner), 0) // nres == iota((wide, inner), 1) // hdim).astype(F32)
    head_half = head_mask.astype(BF16)
    diagonal = (iota((nres, wide), 0) == iota((nres, wide), 1) % nres).astype(F32)
    order = natural(iota((nres, nres), 0)) == iota((nres, nres), 1)
    rows_of = iota((cells, cells), 0)
    cols_of = iota((cells, cells), 1)
    block = held * held
    pack = (
        rows_of % held * nres + rows_of // block * held + rows_of // held % held == cols_of
    ).astype(BF16)
    unpack = (
        rows_of // held % group * block + rows_of // nres * held + rows_of % held == cols_of
    ).astype(BF16)

    def expand(values):
        return jnp.concatenate([values] * heads, axis=0) * head_half

    def pick_heads(full):
        kept = full * head_mask
        total = kept[:nres]
        for h in range(1, heads):
            total = total + kept[h * nres : (h + 1) * nres]
        return total

    def flip_heads(values):
        turned = values.T
        return jnp.concatenate(
            [turned[h * nres : (h + 1) * nres] for h in range(heads)], axis=1
        )

    def wide_bias(which):
        rows = bias_ref[which].astype(F32)
        return jnp.concatenate(
            [jnp.broadcast_to(rows[h : h + 1], (nres, channels)) for h in range(heads)],
            axis=0,
        ).astype(BF16)

    def norm(values, which):
        return layer_norm(values, gain_ref[which : which + 1], shift_ref[which : which + 1])

    def split(values):
        return [values[r * nres : (r + 1) * nres] for r in range(held)]

    def bias_rows(normal, spread):
        full = mm(normal, spread, NT)
        rows = [jnp.sum(part * diagonal, axis=0, keepdims=True) for part in split(full)]
        return jnp.concatenate(rows, axis=0).astype(BF16).astype(F32)

    def project(normal, which):
        queries = (mm(normal, proj_ref[which, 0], NN) * scale).astype(BF16)
        keys = mm(normal, proj_ref[which, 1], NN).astype(BF16)
        values = mm(normal, proj_ref[which, 2], NN).astype(BF16)
        gate = jax.nn.sigmoid(
            mm(normal, proj_ref[which, 3], NN) + gate_ref[which : which + 1]
        )
        wide_queries = [expand(part) for part in split(queries)]
        key_parts = split(keys)
        logits = [mm(k, q, NT) + key_bias for k, q in zip(key_parts, wide_queries)]
        return key_parts, split(values), gate, wide_queries, logits

    def attend(parts, bias):
        keys, values, gate, wide_queries, logits = parts
        probs, halves, attended = [], [], []
        for r in range(held):
            scores = logits[r] + bias
            weights = jnp.exp(scores - jnp.max(scores, axis=0, keepdims=True))
            probs.append(weights / jnp.sum(weights, axis=0, keepdims=True))
            halves.append(probs[r].astype(BF16))
            attended.append(pick_heads(mm(halves[r], values[r], TN)))
        attended = jnp.concatenate(attended, axis=0)
        gated = (gate * attended).astype(BF16)
        return probs, halves, attended, gated

    def logit_grads(parts, soft, grad_gated):
        keys, values, gate, wide_queries, unused = parts
        probs, halves, attended, gated = soft
        wide_grads = [expand(part) for part in split((grad_gated * gate).astype(BF16))]
        grad_pre = (grad_gated * attended * gate * (1.0 - gate)).astype(BF16)
        bias_sum, logit_halves = None, []
        for r in range(held):
            grad_probs = mm(values[r], wide_grads[r], NT)
            grad_logits = probs[r] * (
                grad_probs - jnp.sum(probs[r] * grad_probs, axis=0, keepdims=True)
            )
            bias_sum = grad_logits if r == 0 else bias_sum + grad_logits
            logit_halves.append(grad_logits.astype(BF16))
        return bias_sum, (wide_grads, grad_pre, logit_halves)

    def value_grads(soft, wide_grads):
        parts = [mm(half, wide, NN).astype(BF16) for half, wide in zip(soft[1], wide_grads)]
        return jnp.concatenate(parts, axis=0)

    def query_key_grads(parts, logit_halves):
        keys, values, gate, wide_queries, unused = parts
        queries_out, keys_out = [], []
        for r in range(held):
            queries_out.append((pick_heads(mm(logit_halves[r], keys[r], TN)) * scale).astype(BF16))
            keys_out.append(mm(logit_halves[r], wide_queries[r], NN).astype(BF16))
        return [jnp.concatenate(queries_out, axis=0), jnp.concatenate(keys_out, axis=0)]

    def join(grads, which):
        total = mm(grads[0], proj_ref[which, 0], NT)
        for m in range(1, 4):
            total = total + mm(grads[m], proj_ref[which, m], NT)
        return total

    def stage_matrix(slot, tile, matrix):
        half = matrix.astype(BF16)
        for r in range(matrix.shape[0] // TILE):
            stage_w[slot, tile % group, tile // group] = half[r * TILE : (r + 1) * TILE]
            tile += 1

    tiles = channels // TILE
    early = pl.ds(0, 3 * tiles // group)
    late = pl.ds(3 * tiles // group, 2 * tiles // group)

    def stage_early(normal, grads, gated, grad_out, slot):
        stage_matrix(slot, 0, mm(gated, grad_out, TN))
        stage_matrix(slot, tiles, mm(normal, grads[3], TN))
        stage_matrix(slot, 2 * tiles, mm(normal, grads[2], TN))

    def stage_late(normal, grads, slot):
        stage_matrix(slot, 3 * tiles, mm(normal, grads[0], TN))
        stage_matrix(slot, 4 * tiles, mm(normal, grads[1], TN))

    def bias_back(normal, spread, total):
        rounded = total.astype(BF16).astype(F32)
        placed = jnp.concatenate(
            [rounded[r : r + 1] * diagonal for r in range(held)], axis=0
        ).astype(BF16)
        grown = mm(placed, spread, NN)
        by_cell = mm(placed, normal, TN)
        rows = [
            jnp.sum(by_cell[h * nres : (h + 1) * nres], axis=0, keepdims=True)
            for h in range(heads)
        ]
        return grown, rows

    def stage_sums(which, rows, grad_pre, grad_normal, normed):
        rows = rows + [
            jnp.sum(grad_pre.astype(F32), axis=0, keepdims=True),
            jnp.sum(grad_normal * normed, axis=0, keepdims=True),
            jnp.sum(grad_normal, axis=0, keepdims=True),
        ]
        spare = stage_small.shape[1] - len(rows)
        if spare:
            rows = rows + [jnp.zeros((spare, channels), F32)]
        rows = jnp.concatenate(rows, axis=0)
        stage_small[which] = rows
        got_small[which, seat] = rows

    def send_weights(slot, part, channel):
        got_w[slot, seat, part] = stage_w[slot, seat, part]
        send(lambda other: stage_w.at[slot, other, part], got_w.at[slot], channel, part=part)

    def pass_weights(slot, part, channel, next_channel):
        received(got_w.at[slot], channel, part)
        total = jnp.sum(got_w[slot, :, part].astype(F32), axis=0).astype(BF16)
        own_w[slot, part] = total
        weights_out[slot, seat, part] = total
        send(
            lambda other: own_w.at[slot, part], weights_out.at[slot], next_channel, part=part
        )

    order_half = order.astype(BF16)
    loads["pair"].wait()
    pair_own = mm(order_half, pair_ref[0], NN).astype(BF16)
    stage_in[0] = pair_own
    got_in[0, layer] = pair_own
    for name in ("gain", "shift", "bias"):
        loads[name].wait()
    spread0 = wide_bias(0)
    unused_normed, unused_inverse, normal_own = norm(pair_own, 0)
    row0 = jnp.sum(mm(normal_own, spread0, NT) * diagonal, axis=0, keepdims=True)
    row0 = row0.astype(BF16).astype(F32)
    stage_bias[...] = row0
    spot = seat * held + layer
    got_bias[spot] = row0
    loads["cot"].wait()
    cot_own = mm(order_half, cot_ref[0], NN).astype(BF16)
    stage_in[1] = cot_own
    got_in[1, layer] = cot_own
    with jax.named_scope("bar"):
        pl.semaphore_wait(barrier, len(others))
    send(lambda other: stage_in.at[0], got_in.at[0], 0, layer, twins)
    send(lambda other: stage_bias, got_bias, 1, spot, others)
    send(lambda other: stage_in.at[1], got_in.at[1], 12, layer, twins)
    for name in ("mask", "proj", "gate", "out"):
        loads[name].wait()
    key_row = (mask_ref[...].astype(F32) - 1.0) * MASKED
    key_bias = jnp.sum(jnp.where(order, key_row, 0.0), axis=1, keepdims=True)
    spread1 = wide_bias(1)
    received(got_in.at[0], 0)
    first_in = got_in[0].reshape(cells, channels)
    normed0, inverse0, normal0 = norm(first_in, 0)

    parts0 = project(normal0, 0)
    received(got_in.at[1], 12)
    cotangent_half = got_in[1].reshape(cells, channels)
    cotangent = cotangent_half.astype(F32)
    packed_grad = mm(pack, cotangent_half, NN).astype(BF16)
    received(got_bias, 1)
    soft0 = attend(parts0, flip_heads(got_bias[...].reshape(nres, wide)))
    update = mm(soft0[3], out_ref[0], NN).astype(BF16)
    after_first = (first_in.astype(F32) + update.astype(F32)).astype(BF16)
    packed = mm(pack, after_first, NN).astype(BF16)
    packed = jnp.concatenate([packed, packed_grad], axis=1).reshape(group, block, 2 * channels)
    stage_flip[...] = packed
    got_flip[seat] = stage_flip[seat]
    send(lambda other: stage_flip.at[other], got_flip, 2)
    normed1, inverse1, normal1 = norm(after_first, 1)
    row1 = bias_rows(normal1, spread1)
    stage_bias1[...] = row1
    got_bias1[seat] = row1
    send(lambda other: stage_bias1, got_bias1, 3)
    received(got_flip, 2)

    flipped = mm(unpack, got_flip[...].reshape(cells, 2 * channels), NN).astype(BF16)
    column_grad = flipped[:, channels:]
    unused_normed, unused_inverse, normal_col = norm(flipped[:, :channels], 1)
    parts1 = project(normal_col, 1)
    grad_gated1 = mm(column_grad, out_ref[1], NT)
    received(got_bias1, 3)
    soft1 = attend(parts1, got_bias1[...].reshape(nres, wide))
    bias_sum1, found1 = logit_grads(parts1, soft1, grad_gated1)
    stage_sum[1] = bias_sum1.reshape(group, held, wide)
    got_sum[1, seat] = stage_sum[1, seat]
    send(lambda other: stage_sum.at[1, other], got_sum.at[1], 4)
    grads1 = query_key_grads(parts1, found1[2])
    grads1 = grads1 + [value_grads(soft1, found1[0]), found1[1]]
    back = mm(pack, join(grads1, 1).astype(BF16), NN).astype(BF16)
    stage_back[...] = back.reshape(group, block, channels)
    got_back[seat] = stage_back[seat]
    send(lambda other: stage_back.at[other], got_back, 5)
    stage_early(normal_col, grads1, soft1[3], column_grad, 1)
    stage_late(normal_col, grads1, 1)
    every = pl.ds(0, 5 * tiles // group)
    send_weights(1, every, 6)
    received(got_sum.at[1], 4)
    grown1, rows1 = bias_back(normal1, spread1, jnp.sum(got_sum[1], axis=0))
    received(got_back, 5)
    back = mm(unpack, got_back[...].reshape(cells, channels), NN)
    grad_normal1 = back + grown1
    end_grad = norm_backward(grad_normal1, normed1, inverse1, gain_ref[1:2])
    grad_after = cotangent + end_grad.astype(BF16).astype(F32)
    grad_after_half = grad_after.astype(BF16)

    grad_gated0 = mm(grad_after_half, out_ref[0], NT)
    bias_sum0, found0 = logit_grads(parts0, soft0, grad_gated0)
    stage_sum[0] = flip_heads(bias_sum0).reshape(group, held, wide)
    got_sum[0, seat] = stage_sum[0, seat]
    value0 = value_grads(soft0, found0[0])
    stage_early(normal0, [None, None, value0, found0[1]], soft0[3], grad_after_half, 0)
    send(lambda other: stage_sum.at[0, other], got_sum.at[0], 7)
    send_weights(0, early, 8)
    grads0 = query_key_grads(parts0, found0[2]) + [value0, found0[1]]
    stage_late(normal0, grads0, 0)
    send_weights(0, late, 14)
    stage_sums(1, rows1, grads1[3], grad_normal1, normed1)
    send(lambda other: stage_small.at[1], got_small.at[1], 13)
    pass_weights(1, every, 6, 9)
    joined0 = join(grads0, 0)
    received(got_sum.at[0], 7)
    grown0, rows0 = bias_back(normal0, spread0, jnp.sum(got_sum[0], axis=0))
    grad_normal0 = grown0 + joined0
    stage_sums(0, rows0, grads0[3], grad_normal0, normed0)
    send(lambda other: stage_small.at[0], got_small.at[0], 10)
    pass_weights(0, early, 8, 11)
    pass_weights(0, late, 14, 15)
    start_grad = norm_backward(grad_normal0, normed0, inverse0, gain_ref[0:1])
    result[...] = (grad_after + start_grad).reshape(held, nres, channels)
    kept = result[layer]
    for p in range(nres):
        i = p % held * group + p // held
        pair_out[0, i : i + 1] = kept[p : p + 1]
    received(got_small.at[1], 13)
    small_out[1] = jnp.sum(got_small[1], axis=0)
    received(weights_out.at[1], 9, every)
    received(got_small.at[0], 10)
    small_out[0] = jnp.sum(got_small[0], axis=0)
    received(weights_out.at[0], 11, early)
    received(weights_out.at[0], 15, late)
    with jax.named_scope("ends"):
        for target, channel, part in waits:
            wait_all(target, send_sem.at[channel], part)


def finish_kernel(
    heads,
    pair_in,
    weights_in,
    small_in,
    pair_out,
    proj_out,
    gate_out,
    outw_out,
    biasw_out,
    gain_out,
    shift_out,
):
    group = weights_in.shape[1]
    pair_out[...] = pair_in[...]
    for which in range(2):
        tile = 0
        for m in (4, 3, 2, 0, 1):
            for r in range(proj_out.shape[2] // TILE):
                piece = weights_in[which, tile % group, tile // group].astype(F32)
                if m < 4:
                    proj_out[which, m, r * TILE : (r + 1) * TILE] = piece
                else:
                    outw_out[which, r * TILE : (r + 1) * TILE] = piece
                tile += 1
        small = small_in[which]
        biasw_out[which] = small[:heads]
        gate_out[which : which + 1] = small[heads : heads + 1]
        gain_out[which : which + 1] = small[heads + 1 : heads + 2]
        shift_out[which : which + 1] = small[heads + 2 : heads + 3]


def fused(
    row_count,
    head_count,
    pair_input,
    cotangent,
    residue_mask,
    norm_gain,
    norm_shift,
    proj_weights,
    gate_bias,
    out_weights,
    bias_weights,
):
    n = row_count * head_count
    held = RESIDENT
    group = n // held
    nres, channels = pair_input.shape[1:]
    heads = bias_weights.shape[2]
    slots = 5 * channels // TILE // group
    wide = heads * nres
    block = held * held
    small = -(-(heads + 3) // 8) * 8
    shape = jax.ShapeDtypeStruct
    vmem = pl.BlockSpec(memory_space=pltpu.VMEM)
    far = pl.BlockSpec(memory_space=pltpu.HBM)
    inputs = (
        pair_input,
        cotangent,
        residue_mask.reshape(1, -1),
        norm_gain,
        norm_shift,
        proj_weights,
        gate_bias,
        out_weights,
        bias_weights.transpose(0, 2, 1),
    )
    parts = pl.pallas_call(
        functools.partial(fused_kernel, head_count, held, group, heads),
        out_shape=(
            shape(pair_input.shape, F32),
            shape((2, group, slots, TILE, channels), BF16),
            shape((2, small, channels), F32),
        ),
        in_specs=[far] * len(inputs),
        out_specs=[vmem] * 3,
        scratch_shapes=[pltpu.VMEM(each.shape, each.dtype) for each in inputs]
        + [
            pltpu.VMEM((2, nres, channels), BF16),
            pltpu.VMEM((2, held, nres, channels), BF16),
            pltpu.VMEM((1, wide), F32),
            pltpu.VMEM((n, 1, wide), F32),
            pltpu.VMEM((group, block, 2 * channels), BF16),
            pltpu.VMEM((group, block, 2 * channels), BF16),
            pltpu.VMEM((held, wide), F32),
            pltpu.VMEM((group, held, wide), F32),
            pltpu.VMEM((group, block, channels), BF16),
            pltpu.VMEM((group, block, channels), BF16),
            pltpu.VMEM((2, group, held, wide), F32),
            pltpu.VMEM((2, group, held, wide), F32),
            pltpu.VMEM((2, group, slots, TILE, channels), BF16),
            pltpu.VMEM((2, group, slots, TILE, channels), BF16),
            pltpu.VMEM((2, slots, TILE, channels), BF16),
            pltpu.VMEM((2, small, channels), F32),
            pltpu.VMEM((2, group, small, channels), F32),
            pltpu.VMEM((held, nres, channels), F32),
            pltpu.SemaphoreType.DMA((16,)),
            pltpu.SemaphoreType.DMA((16,)),
            pltpu.SemaphoreType.DMA((len(inputs),)),
        ],
        compiler_params=pltpu.CompilerParams(
            collective_id=0, has_side_effects=True, vmem_limit_bytes=VMEM_GRANT
        ),
    )(*(pltpu.with_memory_space_constraint(each, pltpu.HBM) for each in inputs))
    outs = pl.pallas_call(
        functools.partial(finish_kernel, heads),
        out_shape=(
            shape(pair_input.shape, F32),
            shape(proj_weights.shape, F32),
            shape(gate_bias.shape, F32),
            shape(out_weights.shape, F32),
            shape((2, heads, channels), F32),
            shape(norm_gain.shape, F32),
            shape(norm_shift.shape, F32),
        ),
        in_specs=[vmem] * 3,
        out_specs=[vmem] * 7,
        compiler_params=pltpu.CompilerParams(vmem_limit_bytes=VMEM_GRANT),
    )(*parts)
    outs = list(outs)
    outs[4] = outs[4].transpose(0, 2, 1)
    return tuple(outs)


def dispatch(row_count, head_count, *arrays):
    pair_input, proj_weights, bias_weights = arrays[0], arrays[5], arrays[8]
    rows, residues, channels = pair_input.shape
    inner = proj_weights.shape[3]
    wide = bias_weights.shape[2] * residues
    group = row_count * head_count // RESIDENT
    fits = (
        rows == 1
        and residues == group * RESIDENT
        and wide == inner == channels
        and channels % (TILE * group) == 0
        and group & (group - 1) == 0
        and group % head_count == 0
    )
    if fits:
        return fused(row_count, head_count, *arrays)
    return local(*arrays)


def solution(mesh):
    return jax.shard_map(
        functools.partial(dispatch, mesh.shape["row"], mesh.shape["head"]),
        mesh=mesh,
        in_specs=(
            P(("row", "head"), None, None),
            P(("row", "head"), None, None),
            P(),
            P(),
            P(),
            P(),
            P(),
            P(),
            P(),
        ),
        out_specs=(P(("row", "head"), None, None), P(), P(), P(), P(), P(), P()),
        check_vma=False,
    )
```
